32 devices in a mesh: row: 4 (over y, core), col: 8 (over z, x).
Axes of the slice: x: 2, y: 2, z: 4, core: 2. Of those that a mesh axis runs over, the one named last changes fastest.
Arguments:
- coupling_panel: bfloat16 [4, 1536, 512], P('row'), may hold values from -6 to 6
- interior_factor: float32 [4, 1536, 1536], P('row'), may hold values from -1 to 3, as said below
- border_rows: bfloat16 [4, 4096, 1536], P('row', 'col'), may hold values from -0.109375 to 0.109375
- target_rows: int32 [4, 4096], P('row', 'col'), may hold values from 0 to 8191, as said below
- border_block: float32 [8192, 512], P(('row', 'col')), may hold values from -6 to 6
Outputs:
- schur_panel: float32 [8192, 512], P(('row', 'col'))
The draws below stay inside these ranges and needn't reach their ends.
Inputs may be any that keep to these rules, and one draw needn't show every extreme that they name: `target_rows`: each block of 512 entries along the second dimension (the rows of one device) is nondecreasing. Row g of the Schur panel is held by device g // 256 in the order of row+col. The rows of one device name any one holder at most 32 times, and some holder is named exactly 32 times by the rows of every device. `interior_factor`: each [1536, 1536] block is lower triangular with diagonal entries between 1 and 3.
All inputs are finite; a program needn't handle non-finite values.
Results may differ from the reference program's by a relative error of at most 0.0029.
Values may be sent and summed in bfloat16 or wider, within the bound.
A program may use at most 128 MiB of HBM per device.

```python
import jax
import jax.numpy as jnp
from jax import lax

PANEL = 512
INTERIOR = 1536
BORDER_DEV = 512
OWNED_DEV = 256
NI = 8192
DEPTH = 32
SUBTREES = 4
N_ROW = 4
N_COL = 8
DEVICES = 32


def draw_interior_factor(key, part):
    diag_key, lower_key = jax.random.split(key)
    diagonal = jax.random.uniform(diag_key, (SUBTREES, INTERIOR), jnp.float32, 1.0, 2.0)
    off_scale = 2.7
    lower_part = jax.random.normal(lower_key, (SUBTREES, INTERIOR, INTERIOR), jnp.float32)
    lower_part = jnp.clip(jnp.clip(lower_part, -4.0, 4.0) * (off_scale / INTERIOR ** 0.5), -1.0, 1.0)
    strict = jnp.tril(jnp.ones((INTERIOR, INTERIOR), jnp.float32), -1)
    identity = jnp.eye(INTERIOR, dtype=jnp.float32)
    return lower_part * strict[None] + diagonal[:, :, None] * identity[None]


def draw_target_rows(key, part):
    hottest = jax.random.randint(jax.random.fold_in(key, 11), (), 0, DEVICES)
    tiers = jax.random.randint(jax.random.fold_in(key, 12), (DEVICES,), 0, 4)
    others = jnp.arange(DEVICES - 1, dtype=jnp.int32)
    other_owner = others + (others >= hottest).astype(jnp.int32)
    candidates = jnp.arange((DEVICES - 1) * DEPTH, dtype=jnp.int32)
    cand_owner = other_owner[candidates // DEPTH]

    def one_source(source):
        source_key = jax.random.fold_in(key, 100 + source)
        noise = jax.random.randint(source_key, candidates.shape, 0, 16384)
        scores = (tiers[cand_owner] * 4096 + noise) * 8192 + candidates
        unused, chosen = lax.top_k(scores, BORDER_DEV - DEPTH)
        holders = jnp.concatenate([jnp.full((DEPTH,), hottest, jnp.int32), cand_owner[chosen]])
        within = jax.random.randint(jax.random.fold_in(source_key, 7), (BORDER_DEV,), 0, OWNED_DEV)
        return jnp.sort(holders * OWNED_DEV + within)
    flat = jax.vmap(one_source)(jnp.arange(DEVICES, dtype=jnp.int32))
    return flat.reshape(N_ROW, N_COL * BORDER_DEV).astype(jnp.int32)


def block_levels(stream_key, dims, shards, least, largest):
    level = 1.0
    for dim, blocks in shards:
        draws = jax.random.uniform(jax.random.fold_in(jax.random.fold_in(stream_key, 6), dim), (blocks,), jnp.float32, least / len(shards), largest / len(shards))
        level = level * jnp.repeat(jnp.exp(draws), dims[dim] // blocks).reshape((-1,) + (1,) * (len(dims) - 1 - dim))
    return level


def scatter_about(rng, extent, width, limit, cuts=(), kind=jnp.bfloat16):
    result = width * jax.random.normal(rng, extent, jnp.float32)
    if cuts:
        result = result * block_levels(rng, extent, cuts, -0.22, 0.18)
    return jnp.clip(result, -limit, limit).astype(kind)


def setup_inputs(seed: int = 0) -> dict:
    key_of = jax.random.split(jax.random.key(seed), 6)
    return {
        "coupling_panel": scatter_about(key_of[0], (SUBTREES, INTERIOR, PANEL), 1.0, 6.0, ((0, 4),)),
        "interior_factor": draw_interior_factor(jax.random.fold_in(key_of[5], 71), 0),
        "border_rows": scatter_about(key_of[2], (SUBTREES, N_COL * BORDER_DEV, INTERIOR), (2 * INTERIOR) ** -0.5, 0.109375, ((0, 4), (1, 8))),
        "target_rows": draw_target_rows(jax.random.fold_in(key_of[5], 71), 0),
        "border_block": scatter_about(key_of[4], (NI, PANEL), 1.0, 6.0, ((0, 32),), jnp.float32),
    }


def substitute(factor, panel_cols):
    forward = lax.linalg.triangular_solve(factor, panel_cols, left_side=True, lower=True)
    return lax.linalg.triangular_solve(factor, forward, left_side=True, lower=True, transpose_a=True)

def reference(coupling_panel, interior_factor, border_rows, target_rows, border_block):

    def subtree(assembled, pieces):
        panel_cols, factor, coupling_rows, targets = pieces
        solved = substitute(factor, panel_cols.astype(jnp.float32)).astype(jnp.bfloat16)
        update = jnp.dot(coupling_rows.astype(jnp.float32), solved.astype(jnp.float32), preferred_element_type=jnp.float32)
        return (assembled.at[targets.astype(jnp.int32)].add(update), None)
    initial = jnp.zeros(border_block.shape, jnp.float32)
    assembled, unused = lax.scan(subtree, initial, (coupling_panel, interior_factor, border_rows, target_rows))
    return border_block - assembled
```

```python
import functools

import jax
import jax.numpy as jnp
from jax import lax
from jax.experimental import pallas as pl
from jax.experimental.pallas import tpu as pltpu
from jax.sharding import PartitionSpec as P

F32 = jnp.float32
BF16 = jnp.bfloat16
BASE = 16
LANES = 128
BLOCK = 256
NN = (((1,), (0,)), ((), ()))
TN = (((0,), (0,)), ((), ()))


def iota(shape, dim):
    return lax.broadcasted_iota(jnp.int32, shape, dim)


def split(x):
    high = x.astype(BF16)
    return high, (x - high.astype(F32)).astype(BF16)


def dot(a, b, dims=NN):
    return lax.dot_general(a, b, dims, preferred_element_type=F32)


def dot3(a, b, dims=NN):
    return dot(a[0], b[0], dims) + (dot(a[0], b[1], dims) + dot(a[1], b[0], dims))


def invert_bases(factor_ref, small_ref):
    chunks = factor_ref.shape[0] // LANES
    padded = small_ref.shape[1]
    small_ref[...] = jnp.ones(small_ref.shape, F32)
    same = iota((LANES, LANES), 0) // BASE == iota((LANES, LANES), 1) // BASE
    for k in range(chunks):
        here = pl.ds(k * LANES, LANES)
        diag = jnp.where(same, factor_ref[here, here], 0.0)
        small_ref[:, k, :] = jnp.sum(diag.reshape(LANES // BASE, BASE, LANES), axis=0)
    rows = small_ref[...].reshape(BASE * padded, LANES)
    high = rows.astype(BF16)
    rest = rows - high.astype(F32)
    mid = rest.astype(BF16)
    low = (rest - mid.astype(F32)).astype(BF16)
    pair = jnp.concatenate([high, mid], axis=1)
    lane = iota((padded, LANES), 1) % BASE
    source = iota((2 * LANES, LANES), 0) % LANES
    target = iota((2 * LANES, LANES), 1)
    solved = []
    coefs = []
    for j in range(BASE):
        spread = ((source // BASE == target // BASE) & (source % BASE == j)).astype(BF16)
        first = j * padded
        coefs.append(dot(pair[first:], spread) + dot(low[first:], spread[:LANES]))
    for i in range(BASE):
        acc = (lane == i).astype(F32)
        for j in range(i):
            at = (i - j) * padded
            acc -= coefs[j][at : at + padded] * solved[j]
        solved.append(acc / coefs[i][:padded])
    for i in range(BASE):
        small_ref[i] = solved[i]


def invert_blocks(factor_ref, small_ref, inv_hi, inv_lo):
    blocks = factor_ref.shape[0] // BLOCK
    row, col = iota((BLOCK, BLOCK), 0), iota((BLOCK, BLOCK), 1)
    per = BLOCK // LANES
    inverses = []
    for p in range(blocks):
        parts = []
        for h in range(per):
            compact = small_ref[:, p * per + h, :]
            parts.append(jnp.concatenate([compact] * (LANES // BASE), axis=0))
        tall = jnp.concatenate(parts, axis=0)
        wide = jnp.concatenate([tall] * per, axis=1)
        inverses.append(jnp.where(row // BASE == col // BASE, wide, 0.0))
    size = BASE
    while size < BLOCK:
        off = (row // (2 * size) == col // (2 * size)) & (row // size != col // size) & (row > col)
        for p in range(blocks):
            here = pl.ds(p * BLOCK, BLOCK)
            below = split(jnp.where(off, factor_ref[here, here], 0.0))
            inverse = split(inverses[p])
            inverses[p] = inverses[p] - dot3(inverse, split(dot3(below, inverse)))
        size *= 2
    for p in range(blocks):
        inv_hi[p], inv_lo[p] = split(inverses[p])


def split_factor(factor_ref, l_hi, l_lo):
    blocks = factor_ref.shape[0] // BLOCK
    for k in range(1, blocks):
        at = (pl.ds(k * BLOCK, BLOCK), pl.ds(0, k * BLOCK))
        l_hi[at], l_lo[at] = split(factor_ref[at])


def substitute(panel, l_hi, l_lo, inv_hi, inv_lo, x_hi, x_lo):
    blocks = inv_hi.shape[0]
    for k in range(blocks):
        here, done = pl.ds(k * BLOCK, BLOCK), pl.ds(0, k * BLOCK)
        acc = panel(here).astype(F32)
        if k:
            acc -= dot3((l_hi[here, done], l_lo[here, done]), (x_hi[done, :], x_lo[done, :]))
        x_hi[here, :], x_lo[here, :] = split(dot3((inv_hi[k], inv_lo[k]), split(acc)))
    for k in reversed(range(blocks)):
        here = pl.ds(k * BLOCK, BLOCK)
        done = pl.ds((k + 1) * BLOCK, (blocks - 1 - k) * BLOCK)
        acc = x_hi[here, :].astype(F32) + x_lo[here, :].astype(F32)
        if k < blocks - 1:
            acc -= dot3((l_hi[done, here], l_lo[done, here]), (x_hi[done, :], x_lo[done, :]), TN)
        x_hi[here, :], x_lo[here, :] = split(dot3((inv_hi[k], inv_lo[k]), split(acc), TN))


def slots_of(targets, holders, depth, owned):
    rows = targets.shape[1]
    holder = targets // owned
    ids = iota((holders, rows), 0)
    counts = jnp.sum((ids == holder).astype(F32), axis=1, keepdims=True)
    start = jnp.sum(jnp.where(ids < holder, counts, 0.0), axis=0, keepdims=True).astype(jnp.int32)
    position = holder * depth + iota((1, rows), 1) - start
    return iota((holders * depth, rows), 0) == position


def solve_kernel(holders, depth, owned, factor_ref, panel_ref, border_ref, targets_ref, out_ref,
                 small_ref, inv_hi, inv_lo, l_hi, l_lo, x_hi, x_lo, slots_ref):
    slots = slots_of(targets_ref[...], holders, depth, owned)
    slots_ref[...] = jnp.where(slots, 1.0, 0.0).astype(BF16)
    invert_bases(factor_ref, small_ref)
    invert_blocks(factor_ref, small_ref, inv_hi, inv_lo)
    split_factor(factor_ref, l_hi, l_lo)
    substitute(lambda at: panel_ref[at, :], l_hi, l_lo, inv_hi, inv_lo, x_hi, x_lo)
    update = dot(border_ref[...], x_hi[...]).astype(BF16)
    out_ref[...] = dot(slots_ref[...], update).astype(BF16)


def solve(holders, depth, owned, factor, panel, border, targets):
    n, width = panel.shape
    vmem = pl.BlockSpec(memory_space=pltpu.VMEM)
    padded = -(-(n // LANES) // 8) * 8
    return pl.pallas_call(
        functools.partial(solve_kernel, holders, depth, owned),
        out_shape=jax.ShapeDtypeStruct((holders * depth, width), BF16),
        in_specs=[vmem] * 4,
        out_specs=vmem,
        scratch_shapes=[
            pltpu.VMEM((BASE, padded, LANES), F32),
            pltpu.VMEM((n // BLOCK, BLOCK, BLOCK), BF16),
            pltpu.VMEM((n // BLOCK, BLOCK, BLOCK), BF16),
            pltpu.VMEM((n, n), BF16),
            pltpu.VMEM((n, n), BF16),
            pltpu.VMEM((n, width), BF16),
            pltpu.VMEM((n, width), BF16),
            pltpu.VMEM((holders * depth, border.shape[0]), BF16),
        ],
        compiler_params=pltpu.CompilerParams(vmem_limit_bytes=60 * 2**20),
        cost_estimate=pl.CostEstimate(flops=10**10, bytes_accessed=14 * 10**6, transcendentals=0),
        name="solve",
    )(factor, panel, border, targets)


def gather_kernel(owned, index_ref, received_ref, block_ref, out_ref):
    slots = received_ref.shape[0]
    pick = iota((owned, slots), 0) == index_ref[...]
    pick = jnp.where(pick, 1.0, 0.0).astype(BF16)
    out_ref[...] = block_ref[...] - dot(pick, received_ref[...])


def gather(index, received, block):
    vmem = pl.BlockSpec(memory_space=pltpu.VMEM)
    return pl.pallas_call(
        functools.partial(gather_kernel, block.shape[0]),
        out_shape=jax.ShapeDtypeStruct(block.shape, F32),
        in_specs=[vmem] * 3,
        out_specs=vmem,
        compiler_params=pltpu.CompilerParams(vmem_limit_bytes=40 * 2**20),
        name="gather",
    )(index, received, block)


def local(coupling_panel, interior_factor, border_rows, target_rows, border_block):
    holders = lax.axis_size("row") * lax.axis_size("col")
    owned = border_block.shape[0]
    targets = target_rows[0]
    sent = targets.shape[0]
    depth = 2 * sent // holders
    width = border_block.shape[1]
    holder_of = targets // owned
    ids = jnp.arange(holders, dtype=jnp.int32)
    start = jnp.sum((holder_of[None, :] < ids[:, None]).astype(jnp.int32), axis=1)
    first = start[:, None] + jnp.arange(depth, dtype=jnp.int32)[None, :]
    wanted = targets[jnp.minimum(first, sent - 1)]
    valid = (first < sent) & (wanted // owned == ids[:, None])
    send_index = jnp.where(valid, wanted % owned, -1)
    recv_index = lax.all_to_all(send_index, ("row", "col"), split_axis=0, concat_axis=0, tiled=True)
    outgoing = solve(holders, depth, owned, interior_factor[0], coupling_panel[0], border_rows[0], target_rows)
    received = lax.all_to_all(
        outgoing.reshape(holders, depth, width), ("row", "col"), split_axis=0, concat_axis=0, tiled=True
    )
    return gather(recv_index.reshape(1, -1), received.reshape(holders * depth, width), border_block)


def solution(mesh):
    placed = (
        P("row", None, None),
        P("row", None, None),
        P("row", "col", None),
        P("row", "col"),
        P(("row", "col"), None),
    )
    return jax.shard_map(
        local, mesh=mesh, in_specs=placed, out_specs=P(("row", "col"), None), check_vma=False
    )
```

```python
import functools

import jax
import jax.numpy as jnp
from jax import lax
from jax.experimental import pallas as pl
from jax.experimental.pallas import tpu as pltpu
from jax.sharding import PartitionSpec as P

F32 = jnp.float32
BF16 = jnp.bfloat16
BASE = 16
LANES = 128
BLOCK = 256
COLUMNS = 256
NN = (((1,), (0,)), ((), ()))
TN = (((0,), (0,)), ((), ()))


def iota(shape, dim):
    return lax.broadcasted_iota(jnp.int32, shape, dim)


def split(x):
    high = x.astype(BF16)
    return high, (x - high.astype(F32)).astype(BF16)


def dot(a, b, dims=NN):
    return lax.dot_general(a, b, dims, preferred_element_type=F32)


def dot3(a, b, dims=NN):
    return dot(a[0], b[0], dims) + (dot(a[0], b[1], dims) + dot(a[1], b[0], dims))


def invert_bases(factor_ref, small_ref):
    chunks = factor_ref.shape[0] // LANES
    padded = small_ref.shape[1]
    small_ref[...] = jnp.ones(small_ref.shape, F32)
    same = iota((LANES, LANES), 0) // BASE == iota((LANES, LANES), 1) // BASE
    for k in range(chunks):
        here = pl.ds(k * LANES, LANES)
        diag = jnp.where(same, factor_ref[here, here], 0.0)
        small_ref[:, k, :] = jnp.sum(diag.reshape(LANES // BASE, BASE, LANES), axis=0)
    rows = small_ref[...].reshape(BASE * padded, LANES)
    high = rows.astype(BF16)
    rest = rows - high.astype(F32)
    mid = rest.astype(BF16)
    low = (rest - mid.astype(F32)).astype(BF16)
    pair = jnp.concatenate([high, mid], axis=1)
    lane = iota((padded, LANES), 1) % BASE
    source = iota((2 * LANES, LANES), 0) % LANES
    target = iota((2 * LANES, LANES), 1)
    solved = []
    coefs = []
    for j in range(BASE):
        spread = ((source // BASE == target // BASE) & (source % BASE == j)).astype(BF16)
        first = j * padded
        coefs.append(dot(pair[first:], spread) + dot(low[first:], spread[:LANES]))
    for i in range(BASE):
        acc = (lane == i).astype(F32)
        for j in range(i):
            at = (i - j) * padded
            acc -= coefs[j][at : at + padded] * solved[j]
        solved.append(acc / coefs[i][:padded])
    for i in range(BASE):
        small_ref[i] = solved[i]


def invert_blocks(factor_ref, small_ref, inv_hi, inv_lo):
    blocks = factor_ref.shape[0] // BLOCK
    row, col = iota((BLOCK, BLOCK), 0), iota((BLOCK, BLOCK), 1)
    per = BLOCK // LANES
    inverses = []
    for p in range(blocks):
        parts = []
        for h in range(per):
            compact = small_ref[:, p * per + h, :]
            parts.append(jnp.concatenate([compact] * (LANES // BASE), axis=0))
        tall = jnp.concatenate(parts, axis=0)
        wide = jnp.concatenate([tall] * per, axis=1)
        inverses.append(jnp.where(row // BASE == col // BASE, wide, 0.0))
    size = BASE
    while size < BLOCK:
        off = (row // (2 * size) == col // (2 * size)) & (row // size != col // size) & (row > col)
        for p in range(blocks):
            here = pl.ds(p * BLOCK, BLOCK)
            below = split(jnp.where(off, factor_ref[here, here], 0.0))
            inverse = split(inverses[p])
            inverses[p] = inverses[p] - dot3(inverse, split(dot3(below, inverse)))
        size *= 2
    for p in range(blocks):
        inv_hi[p], inv_lo[p] = split(inverses[p])


def split_factor(factor_ref, l_hi, l_lo):
    blocks = factor_ref.shape[0] // BLOCK
    for k in range(1, blocks):
        at = (pl.ds(k * BLOCK, BLOCK), pl.ds(0, k * BLOCK))
        l_hi[at], l_lo[at] = split(factor_ref[at])


def substitute(panel, l_hi, l_lo, inv_hi, inv_lo, x_hi, x_lo):
    blocks = inv_hi.shape[0]
    for k in range(blocks):
        here, done = pl.ds(k * BLOCK, BLOCK), pl.ds(0, k * BLOCK)
        acc = panel(here).astype(F32)
        if k:
            acc -= dot3((l_hi[here, done], l_lo[here, done]), (x_hi[done, :], x_lo[done, :]))
        x_hi[here, :], x_lo[here, :] = split(dot3((inv_hi[k], inv_lo[k]), split(acc)))
    for k in reversed(range(blocks)):
        here = pl.ds(k * BLOCK, BLOCK)
        done = pl.ds((k + 1) * BLOCK, (blocks - 1 - k) * BLOCK)
        acc = x_hi[here, :].astype(F32) + x_lo[here, :].astype(F32)
        if k < blocks - 1:
            acc -= dot3((l_hi[done, here], l_lo[done, here]), (x_hi[done, :], x_lo[done, :]), TN)
        x_hi[here, :], x_lo[here, :] = split(dot3((inv_hi[k], inv_lo[k]), split(acc), TN))


def slots_of(targets, holders, depth, owned):
    rows = targets.shape[1]
    holder = targets // owned
    ids = iota((holders, rows), 0)
    here = ids == holder
    counts = jnp.sum(here.astype(F32), axis=1, keepdims=True)
    start = jnp.sum(jnp.where(ids < holder, counts, 0.0), axis=0, keepdims=True).astype(jnp.int32)
    rank = iota((1, rows), 1) - start
    return holder * depth + rank, here, rank


def flatten(blocks):
    holders, depth, width = blocks.shape
    if depth % 16:
        return blocks.astype(F32).reshape(holders * depth, width).astype(blocks.dtype)
    return blocks.reshape(holders * depth, width)


def panel_kernel(dims, factor_hbm, panel_hbm, border_hbm, targets_ref, block_hbm, out_ref,
                 factor_ref, panel_ref, border_ref, block_ref, small_ref, inv_hi, inv_lo, l_hi, l_lo,
                 x_hi, x_lo, slots_ref, index_out, index_in, send_buf, recv_buf,
                 load_sem, index_send, index_recv, send_sem, recv_sem):
    n_row, n_col, depth = dims
    holders = n_row * n_col
    owned = block_ref.shape[0]
    blocks = inv_hi.shape[0]
    chunks, width = send_buf.shape[0], send_buf.shape[3]
    me = lax.axis_index("row") * n_col + lax.axis_index("col")

    def peer(step):
        other = lax.rem(me + step, holders)
        return other, (other // n_col, lax.rem(other, n_col))

    barrier = pltpu.get_barrier_semaphore()

    def greet(step, carry):
        pl.semaphore_signal(barrier, inc=1, device_id=peer(step)[1], device_id_type=pl.DeviceIdType.MESH)
        return carry

    lax.fori_loop(1, holders, greet, 0)
    diagonal, below = [], []
    for k in range(blocks):
        at = (pl.ds(k * BLOCK, BLOCK), pl.ds(k * BLOCK, BLOCK))
        diagonal.append(pltpu.make_async_copy(factor_hbm.at[at], factor_ref.at[at], load_sem.at[k]))
    for k in range(1, blocks):
        at = (pl.ds(k * BLOCK, BLOCK), pl.ds(0, k * BLOCK))
        below.append(pltpu.make_async_copy(factor_hbm.at[at], factor_ref.at[at], load_sem.at[blocks + k]))
    panel_copy = pltpu.make_async_copy(panel_hbm, panel_ref, load_sem.at[blocks])
    border_copy = pltpu.make_async_copy(border_hbm, border_ref, load_sem.at[2 * blocks])
    block_copy = pltpu.make_async_copy(block_hbm, block_ref, load_sem.at[2 * blocks + 1])
    for copy in diagonal + below + [panel_copy, border_copy, block_copy]:
        copy.start()

    position, here, rank = slots_of(targets_ref[...], holders, depth, owned)
    rows = position.shape[1]
    slots_ref[...] = jnp.where(iota((holders * depth, rows), 0) == position, 1.0, 0.0).astype(BF16)
    within = (lax.rem(targets_ref[...], owned) + 1).astype(F32)
    named = split(jnp.where(here, within, 0.0))
    ranked = jnp.where(iota((LANES, rows), 0) % depth == rank, 1.0, 0.0).astype(BF16)
    nt = (((1,), (1,)), ((), ()))
    index = dot(named[0], ranked, nt) + dot(named[1], ranked, nt)
    index_out[...] = jnp.broadcast_to(index[:, None, :], index_out.shape)

    for copy in diagonal:
        copy.wait()
    invert_bases(factor_ref, small_ref)
    invert_blocks(factor_ref, small_ref, inv_hi, inv_lo)
    for copy in below:
        copy.wait()
    split_factor(factor_ref, l_hi, l_lo)

    pl.semaphore_wait(barrier, holders - 1)

    def index_copy(step):
        other, place = peer(step)
        return pltpu.make_async_remote_copy(
            src_ref=index_out.at[other], dst_ref=index_in.at[me],
            send_sem=index_send.at[other], recv_sem=index_recv.at[me],
            device_id=place, device_id_type=pl.DeviceIdType.MESH,
        )

    def row_copy(chunk, step):
        other, place = peer(step)
        return pltpu.make_async_remote_copy(
            src_ref=send_buf.at[chunk, other], dst_ref=recv_buf.at[chunk, me],
            send_sem=send_sem.at[chunk, other], recv_sem=recv_sem.at[chunk, me],
            device_id=place, device_id_type=pl.DeviceIdType.MESH,
        )

    def arrival(chunk, step):
        other, place = peer(step)
        return pltpu.make_async_remote_copy(
            src_ref=send_buf.at[chunk, me], dst_ref=recv_buf.at[chunk, other],
            send_sem=send_sem.at[chunk, me], recv_sem=recv_sem.at[chunk, other],
            device_id=place, device_id_type=pl.DeviceIdType.MESH,
        )

    def index_arrival(step):
        other, place = peer(step)
        return pltpu.make_async_remote_copy(
            src_ref=index_out.at[me], dst_ref=index_in.at[other],
            send_sem=index_send.at[me], recv_sem=index_recv.at[other],
            device_id=place, device_id_type=pl.DeviceIdType.MESH,
        )

    def each(act):
        def body(step, carry):
            act(step)
            return carry

        lax.fori_loop(1, holders, body, 0)

    each(lambda step: index_copy(step).start())
    index_in[me] = index_out[me]
    panel_copy.wait()
    border_copy.wait()

    def one_chunk(chunk, carry):
        columns = pl.ds(pl.multiple_of(chunk * width, LANES), width)
        substitute(lambda at: panel_ref[at, columns], l_hi, l_lo, inv_hi, inv_lo, x_hi, x_lo)
        update = dot(border_ref[...], x_hi[...]).astype(BF16)
        packed = dot(slots_ref[...], update).reshape(holders, depth, width)
        send_buf[chunk] = packed.astype(BF16)
        each(lambda step: row_copy(chunk, step).start())
        recv_buf[chunk, me] = send_buf[chunk, me]
        return carry

    lax.fori_loop(0, chunks, one_chunk, 0)

    each(lambda step: index_arrival(step).wait_recv())
    wide = jnp.concatenate([index_in[:, 0, :]] * (holders * depth // LANES), axis=1)
    own = iota(wide.shape, 0) == iota(wide.shape, 1) // depth
    wanted = jnp.sum(jnp.where(own, wide, 0.0), axis=0, keepdims=True)
    pick = (iota((owned, holders * depth), 0) + 1).astype(F32) == wanted
    pick = jnp.where(pick, 1.0, 0.0).astype(BF16)
    block_copy.wait()
    for chunk in range(chunks):
        columns = pl.ds(chunk * width, width)
        each(lambda step: arrival(chunk, step).wait_recv())
        out_ref[:, columns] = block_ref[:, columns] - dot(pick, flatten(recv_buf[chunk]))
    each(lambda step: index_copy(step).wait_send())
    for chunk in range(chunks):
        each(lambda step: row_copy(chunk, step).wait_send())


def local(coupling_panel, interior_factor, border_rows, target_rows, border_block):
    n_row, n_col = lax.axis_size("row"), lax.axis_size("col")
    holders = n_row * n_col
    factor, panel, border = interior_factor[0], coupling_panel[0], border_rows[0]
    n, total = panel.shape
    sent = border.shape[0]
    depth = 2 * sent // holders
    width = min(COLUMNS, total)
    chunks = total // width
    blocks = n // BLOCK
    padded = -(-(n // LANES) // 8) * 8
    hbm = pl.BlockSpec(memory_space=pl.ANY)
    vmem = pl.BlockSpec(memory_space=pltpu.VMEM)
    dma = pltpu.SemaphoreType.DMA
    return pl.pallas_call(
        functools.partial(panel_kernel, (n_row, n_col, depth)),
        out_shape=jax.ShapeDtypeStruct(border_block.shape, F32),
        in_specs=[hbm, hbm, hbm, vmem, hbm],
        out_specs=vmem,
        scratch_shapes=[
            pltpu.VMEM((n, n), F32),
            pltpu.VMEM((n, total), BF16),
            pltpu.VMEM(border.shape, BF16),
            pltpu.VMEM(border_block.shape, F32),
            pltpu.VMEM((BASE, padded, LANES), F32),
            pltpu.VMEM((blocks, BLOCK, BLOCK), BF16),
            pltpu.VMEM((blocks, BLOCK, BLOCK), BF16),
            pltpu.VMEM((n, n), BF16),
            pltpu.VMEM((n, n), BF16),
            pltpu.VMEM((n, width), BF16),
            pltpu.VMEM((n, width), BF16),
            pltpu.VMEM((holders * depth, sent), BF16),
            pltpu.VMEM((holders, 8, LANES), F32),
            pltpu.VMEM((holders, 8, LANES), F32),
            pltpu.VMEM((chunks, holders, depth, width), BF16),
            pltpu.VMEM((chunks, holders, depth, width), BF16),
            dma((2 * blocks + 2,)),
            dma((holders,)),
            dma((holders,)),
            dma((chunks, holders)),
            dma((chunks, holders)),
        ],
        compiler_params=pltpu.CompilerParams(
            vmem_limit_bytes=60 * 2**20, collective_id=0, has_side_effects=True
        ),
        name="schur_panel",
    )(factor, panel, border, target_rows, border_block)


def solution(mesh):
    placed = (
        P("row", None, None),
        P("row", None, None),
        P("row", "col", None),
        P("row", "col"),
        P(("row", "col"), None),
    )
    return jax.shard_map(
        local, mesh=mesh, in_specs=placed, out_specs=P(("row", "col"), None), check_vma=False
    )
```

```python
import functools

import jax
import jax.numpy as jnp
from jax import lax
from jax.experimental import pallas as pl
from jax.experimental.pallas import tpu as pltpu
from jax.sharding import PartitionSpec as P

F32 = jnp.float32
BF16 = jnp.bfloat16
BASE = 16
LANES = 128
BLOCK = 256
COLUMNS = 256
NN = (((1,), (0,)), ((), ()))
TN = (((0,), (0,)), ((), ()))


def iota(shape, dim):
    return lax.broadcasted_iota(jnp.int32, shape, dim)


def split(x):
    high = x.astype(BF16)
    return high, (x - high.astype(F32)).astype(BF16)


def dot(a, b, dims=NN):
    return lax.dot_general(a, b, dims, preferred_element_type=F32)


def dot3(a, b, dims=NN):
    return dot(a[0], b[0], dims) + (dot(a[0], b[1], dims) + dot(a[1], b[0], dims))


def invert_bases(factor_ref, small_ref):
    chunks = factor_ref.shape[0] // LANES
    padded = small_ref.shape[1]
    small_ref[...] = jnp.ones(small_ref.shape, F32)
    same = iota((LANES, LANES), 0) // BASE == iota((LANES, LANES), 1) // BASE
    for k in range(chunks):
        here = pl.ds(k * LANES, LANES)
        diag = jnp.where(same, factor_ref[here, here], 0.0)
        small_ref[:, k, :] = jnp.sum(diag.reshape(LANES // BASE, BASE, LANES), axis=0)
    rows = small_ref[...].reshape(BASE * padded, LANES)
    high = rows.astype(BF16)
    rest = rows - high.astype(F32)
    mid = rest.astype(BF16)
    low = (rest - mid.astype(F32)).astype(BF16)
    pair = jnp.concatenate([high, mid], axis=1)
    lane = iota((padded, LANES), 1) % BASE
    source = iota((2 * LANES, LANES), 0) % LANES
    target = iota((2 * LANES, LANES), 1)
    solved = []
    coefs = []
    for j in range(BASE):
        spread = ((source // BASE == target // BASE) & (source % BASE == j)).astype(BF16)
        first = j * padded
        coefs.append(dot(pair[first:], spread) + dot(low[first:], spread[:LANES]))
    for i in range(BASE):
        acc = (lane == i).astype(F32)
        for j in range(i):
            at = (i - j) * padded
            acc -= coefs[j][at : at + padded] * solved[j]
        solved.append(acc / coefs[i][:padded])
    for i in range(BASE):
        small_ref[i] = solved[i]


def invert_blocks(factor_ref, small_ref, inv_hi, inv_lo):
    chunks = factor_ref.shape[0] // LANES
    row, col = iota((LANES, LANES), 0), iota((LANES, LANES), 1)
    inverses = []
    for k in range(chunks):
        tall = jnp.concatenate([small_ref[:, k, :]] * (LANES // BASE), axis=0)
        inverses.append(jnp.where(row // BASE == col // BASE, tall, 0.0))
    size = BASE
    while size < LANES:
        off = (row // (2 * size) == col // (2 * size)) & (row // size != col // size) & (row > col)
        for k in range(chunks):
            here = pl.ds(k * LANES, LANES)
            below = split(jnp.where(off, factor_ref[here, here], 0.0))
            inverse = split(inverses[k])
            inverses[k] = inverses[k] - dot3(inverse, split(dot3(below, inverse)))
        size *= 2
    none = jnp.zeros((LANES, LANES), BF16)
    for p in range(chunks // 2):
        first, second = split(inverses[2 * p]), split(inverses[2 * p + 1])
        below = factor_ref[pl.ds((2 * p + 1) * LANES, LANES), pl.ds(2 * p * LANES, LANES)]
        corner = split(-dot3(second, split(dot3(split(below), first))))
        for part, ref in enumerate((inv_hi, inv_lo)):
            ref[p, :LANES, :LANES] = first[part]
            ref[p, :LANES, LANES:] = none
            ref[p, LANES:, :LANES] = corner[part]
            ref[p, LANES:, LANES:] = second[part]


def split_factor(factor_ref, l_hi, l_lo):
    blocks = factor_ref.shape[0] // BLOCK
    for k in range(1, blocks):
        at = (pl.ds(k * BLOCK, BLOCK), pl.ds(0, k * BLOCK))
        l_hi[at], l_lo[at] = split(factor_ref[at])


def substitute(panel, l_hi, l_lo, inv_hi, inv_lo, x_hi, x_lo):
    blocks = inv_hi.shape[0]
    for k in range(blocks):
        here, done = pl.ds(k * BLOCK, BLOCK), pl.ds(0, k * BLOCK)
        acc = panel(here).astype(F32)
        if k:
            acc -= dot3((l_hi[here, done], l_lo[here, done]), (x_hi[done, :], x_lo[done, :]))
        x_hi[here, :], x_lo[here, :] = split(dot3((inv_hi[k], inv_lo[k]), split(acc)))
    for k in reversed(range(blocks)):
        here = pl.ds(k * BLOCK, BLOCK)
        done = pl.ds((k + 1) * BLOCK, (blocks - 1 - k) * BLOCK)
        acc = x_hi[here, :].astype(F32) + x_lo[here, :].astype(F32)
        if k < blocks - 1:
            acc -= dot3((l_hi[done, here], l_lo[done, here]), (x_hi[done, :], x_lo[done, :]), TN)
        x_hi[here, :], x_lo[here, :] = split(dot3((inv_hi[k], inv_lo[k]), split(acc), TN))


def slots_of(targets, holders, depth, owned):
    rows = targets.shape[1]
    holder = targets // owned
    ids = iota((holders, rows), 0)
    here = ids == holder
    counts = jnp.sum(here.astype(F32), axis=1, keepdims=True)
    start = jnp.sum(jnp.where(ids < holder, counts, 0.0), axis=0, keepdims=True).astype(jnp.int32)
    rank = iota((1, rows), 1) - start
    return holder * depth + rank, here, rank


def flatten(blocks):
    holders, depth, width = blocks.shape
    if depth % 16:
        return blocks.astype(F32).reshape(holders * depth, width).astype(blocks.dtype)
    return blocks.reshape(holders * depth, width)


def panel_kernel(dims, factor_hbm, panel_hbm, border_hbm, targets_ref, block_hbm, out_ref,
                 factor_ref, panel_ref, border_ref, block_ref, small_ref, inv_hi, inv_lo, l_hi, l_lo,
                 x_hi, x_lo, slots_ref, index_out, index_in, send_buf, recv_buf,
                 load_sem, index_send, index_recv, send_sem, recv_sem):
    n_row, n_col, depth = dims
    holders = n_row * n_col
    owned = block_ref.shape[0]
    blocks = inv_hi.shape[0]
    chunks, width = send_buf.shape[0], send_buf.shape[3]
    me = lax.axis_index("row") * n_col + lax.axis_index("col")

    def peer(step):
        other = lax.rem(me + step, holders)
        return other, (other // n_col, lax.rem(other, n_col))

    barrier = pltpu.get_barrier_semaphore()

    def greet(step, carry):
        pl.semaphore_signal(barrier, inc=1, device_id=peer(step)[1], device_id_type=pl.DeviceIdType.MESH)
        return carry

    lax.fori_loop(1, holders, greet, 0)
    diagonal, below = [], []
    for k in range(blocks):
        at = (pl.ds(k * BLOCK, BLOCK), pl.ds(k * BLOCK, BLOCK))
        diagonal.append(pltpu.make_async_copy(factor_hbm.at[at], factor_ref.at[at], load_sem.at[k]))
    for k in range(1, blocks):
        at = (pl.ds(k * BLOCK, BLOCK), pl.ds(0, k * BLOCK))
        below.append(pltpu.make_async_copy(factor_hbm.at[at], factor_ref.at[at], load_sem.at[blocks + k]))
    panel_copy = pltpu.make_async_copy(panel_hbm, panel_ref, load_sem.at[blocks])
    border_copy = pltpu.make_async_copy(border_hbm, border_ref, load_sem.at[2 * blocks])
    block_copy = pltpu.make_async_copy(block_hbm, block_ref, load_sem.at[2 * blocks + 1])
    for copy in diagonal + below + [panel_copy, border_copy, block_copy]:
        copy.start()

    position, here, rank = slots_of(targets_ref[...], holders, depth, owned)
    rows = position.shape[1]
    slots_ref[...] = jnp.where(iota((holders * depth, rows), 0) == position, 1.0, 0.0).astype(BF16)
    within = (lax.rem(targets_ref[...], owned) + 1).astype(F32)
    named = split(jnp.where(here, within, 0.0))
    ranked = jnp.where(iota((LANES, rows), 0) % depth == rank, 1.0, 0.0).astype(BF16)
    nt = (((1,), (1,)), ((), ()))
    index = dot(named[0], ranked, nt) + dot(named[1], ranked, nt)
    index_out[...] = jnp.broadcast_to(index[:, None, :], index_out.shape)

    for copy in diagonal:
        copy.wait()
    invert_bases(factor_ref, small_ref)
    invert_blocks(factor_ref, small_ref, inv_hi, inv_lo)
    for copy in below:
        copy.wait()
    split_factor(factor_ref, l_hi, l_lo)

    pl.semaphore_wait(barrier, holders - 1)

    def index_copy(step):
        other, place = peer(step)
        return pltpu.make_async_remote_copy(
            src_ref=index_out.at[other], dst_ref=index_in.at[me],
            send_sem=index_send.at[other], recv_sem=index_recv.at[me],
            device_id=place, device_id_type=pl.DeviceIdType.MESH,
        )

    def row_copy(chunk, step):
        other, place = peer(step)
        return pltpu.make_async_remote_copy(
            src_ref=send_buf.at[chunk, other], dst_ref=recv_buf.at[chunk, me],
            send_sem=send_sem.at[chunk, other], recv_sem=recv_sem.at[chunk, me],
            device_id=place, device_id_type=pl.DeviceIdType.MESH,
        )

    def arrival(chunk, step):
        other, place = peer(step)
        return pltpu.make_async_remote_copy(
            src_ref=send_buf.at[chunk, me], dst_ref=recv_buf.at[chunk, other],
            send_sem=send_sem.at[chunk, me], recv_sem=recv_sem.at[chunk, other],
            device_id=place, device_id_type=pl.DeviceIdType.MESH,
        )

    def index_arrival(step):
        other, place = peer(step)
        return pltpu.make_async_remote_copy(
            src_ref=index_out.at[me], dst_ref=index_in.at[other],
            send_sem=index_send.at[me], recv_sem=index_recv.at[other],
            device_id=place, device_id_type=pl.DeviceIdType.MESH,
        )

    def each(act):
        def body(step, carry):
            act(step)
            return carry

        lax.fori_loop(1, holders, body, 0)

    each(lambda step: index_copy(step).start())
    index_in[me] = index_out[me]
    panel_copy.wait()
    border_copy.wait()

    def one_chunk(chunk, carry):
        columns = pl.ds(pl.multiple_of(chunk * width, LANES), width)
        substitute(lambda at: panel_ref[at, columns], l_hi, l_lo, inv_hi, inv_lo, x_hi, x_lo)
        update = dot(border_ref[...], x_hi[...]).astype(BF16)
        packed = dot(slots_ref[...], update).reshape(holders, depth, width)
        send_buf[chunk] = packed.astype(BF16)
        each(lambda step: row_copy(chunk, step).start())
        recv_buf[chunk, me] = send_buf[chunk, me]
        return carry

    lax.fori_loop(0, chunks, one_chunk, 0)

    each(lambda step: index_arrival(step).wait_recv())
    wide = jnp.concatenate([index_in[:, 0, :]] * (holders * depth // LANES), axis=1)
    own = iota(wide.shape, 0) == iota(wide.shape, 1) // depth
    wanted = jnp.sum(jnp.where(own, wide, 0.0), axis=0, keepdims=True)
    pick = (iota((owned, holders * depth), 0) + 1).astype(F32) == wanted
    pick = jnp.where(pick, 1.0, 0.0).astype(BF16)
    block_copy.wait()
    each(lambda step: index_copy(step).wait_send())
    for chunk in range(chunks):
        columns = pl.ds(chunk * width, width)
        each(lambda step: row_copy(chunk, step).wait_send())
        each(lambda step: arrival(chunk, step).wait_recv())
        out_ref[:, columns] = block_ref[:, columns] - dot(pick, flatten(recv_buf[chunk]))


def local(coupling_panel, interior_factor, border_rows, target_rows, border_block):
    n_row, n_col = lax.axis_size("row"), lax.axis_size("col")
    holders = n_row * n_col
    factor, panel, border = interior_factor[0], coupling_panel[0], border_rows[0]
    n, total = panel.shape
    sent = border.shape[0]
    depth = 2 * sent // holders
    width = min(COLUMNS, total)
    chunks = total // width
    blocks = n // BLOCK
    padded = -(-(n // LANES) // 8) * 8
    hbm = pl.BlockSpec(memory_space=pl.ANY)
    vmem = pl.BlockSpec(memory_space=pltpu.VMEM)
    dma = pltpu.SemaphoreType.DMA
    return pl.pallas_call(
        functools.partial(panel_kernel, (n_row, n_col, depth)),
        out_shape=jax.ShapeDtypeStruct(border_block.shape, F32),
        in_specs=[hbm, hbm, hbm, vmem, hbm],
        out_specs=vmem,
        scratch_shapes=[
            pltpu.VMEM((n, n), F32),
            pltpu.VMEM((n, total), BF16),
            pltpu.VMEM(border.shape, BF16),
            pltpu.VMEM(border_block.shape, F32),
            pltpu.VMEM((BASE, padded, LANES), F32),
            pltpu.VMEM((blocks, BLOCK, BLOCK), BF16),
            pltpu.VMEM((blocks, BLOCK, BLOCK), BF16),
            pltpu.VMEM((n, n), BF16),
            pltpu.VMEM((n, n), BF16),
            pltpu.VMEM((n, width), BF16),
            pltpu.VMEM((n, width), BF16),
            pltpu.VMEM((holders * depth, sent), BF16),
            pltpu.VMEM((holders, 8, LANES), F32),
            pltpu.VMEM((holders, 8, LANES), F32),
            pltpu.VMEM((chunks, holders, depth, width), BF16),
            pltpu.VMEM((chunks, holders, depth, width), BF16),
            dma((2 * blocks + 2,)),
            dma((holders,)),
            dma((holders,)),
            dma((chunks, holders)),
            dma((chunks, holders)),
        ],
        compiler_params=pltpu.CompilerParams(
            vmem_limit_bytes=60 * 2**20, collective_id=0, has_side_effects=True
        ),
        name="schur_panel",
    )(factor, panel, border, target_rows, border_block)


def solution(mesh):
    placed = (
        P("row", None, None),
        P("row", None, None),
        P("row", "col", None),
        P("row", "col"),
        P(("row", "col"), None),
    )
    return jax.shard_map(
        local, mesh=mesh, in_specs=placed, out_specs=P(("row", "col"), None), check_vma=False
    )
```
